32 devices in a mesh: expert: 8 (over y, x, core), dp: 4 (over z).
Axes of the slice: x: 2, y: 2, z: 4, core: 2. Of those that a mesh axis runs over, the one named last changes fastest.
Arguments:
- out_grads: bfloat16 [4, 1024, 7168], P('dp', 'expert'), may hold values from -6 to 6
- expert_ids: int32 [4, 1024, 8], P('dp', 'expert'), may hold values from 0 to 63, all different within a row; in each aligned block of 128 rows (0 to 127, 128 to 255, ..., all dimensions but the last counted through in order) at most 24 rows name the same one
- gate_probs: float32 [4, 1024, 8], P('dp', 'expert'), may hold values from 0.05 to 0.5
- hidden_acts: bfloat16 [4, 64, 192, 2048], P('dp', 'expert'), may hold values from -6 to 6
- q_previous: bfloat16 [64, 32, 7168], P('expert'), may hold values from -0.0625 to 0.0625
Outputs:
- new_basis: float32 [64, 32, 2048], P('expert')
- q_update: float32 [64, 32, 7168], P('expert', None, 'dp')
The draws below stay inside these ranges and needn't reach their ends.
Inputs may be any that keep to these rules, and one draw needn't show every extreme that they name: `expert_ids`: each row names 8 different experts; among the rows of one device no expert is named more than 24 times.
All inputs are finite; a program needn't handle non-finite values.
Results may differ from the reference program's by a relative error of at most 0.014.
Values may be sent and summed in bfloat16 or wider, within the bound.
A program may use at most 192 MiB of HBM per device.

```python
import math
import jax
import jax.numpy as jnp
import numpy as np
from jax import lax

D = 7168
FF = 2048
TOP = 8
RANK = 32
TOK_DEV = 128
EXPERTS = 64
CAP = 24
SLOTS = 192
TOK_EXP = 1024
N_EXPERT = 8
N_DP = 4


def steps_of(key, extent, shards, smallest, top_value):
    factor_of, own = 1.0, jax.random.fold_in(key, 6)
    for dim, parts in shards:
        heights = jnp.exp(jax.random.uniform(jax.random.fold_in(own, dim), (parts,), jnp.float32, smallest / len(shards), top_value / len(shards)))
        factor_of = factor_of * jnp.repeat(heights, extent[dim] // parts).reshape([-1 if axis == dim else 1 for axis in range(len(extent))])
    return factor_of


def routed_block(rng, own, number, rows, count, top, limit, skew):
    ranking = jax.random.permutation(rng, count)
    crowded, usual = portions_of(count, rows * top, limit, skew, True), portions_of(count, rows * top, limit, skew, False)
    places = jnp.arange(count)

    def named(tallies, rotation):
        used = int((tallies > 0).sum())
        fixed = max(1, used // 4)
        passed = fixed + (places - fixed + rotation * (used - fixed)) % max(1, count - fixed)
        return jnp.zeros((count,), jnp.int32).at[ranking[jnp.where(places < fixed, places, passed)]].set(jnp.asarray(tallies, jnp.int32))

    tallies = jnp.where(number % 4 == 0, named(crowded, number // 4), named(usual, number - number // 4 - 1))
    mixed = jax.random.permutation(jax.random.fold_in(own, 3), count)
    source_of, sink = mixed[0:count // 2 * 2:2], mixed[1:count // 2 * 2:2]
    room = jnp.minimum(tallies[source_of] - 1, limit - tallies[sink]) // 2
    room = jnp.where((source_of == ranking[0]) | (sink == ranking[0]) | (tallies[sink] == 0), 0, jnp.maximum(room, 0))
    passed = jax.random.randint(jax.random.fold_in(own, 4), (count // 2,), 0, 1 << 20) % (room + 1)
    tallies = tallies.at[source_of].add(-passed).at[sink].add(passed)
    labels = jnp.searchsorted(jnp.cumsum(tallies), jnp.arange(rows * top), side="right").astype(jnp.int32)
    grid = labels.reshape(top, rows).T
    grid = grid[jax.random.permutation(jax.random.fold_in(own, 1), rows)]
    rotation = jax.random.randint(jax.random.fold_in(own, 2), (rows, 1), 0, top)
    return jnp.take_along_axis(grid, (jnp.arange(top)[None, :] + rotation) % top, axis=1)


def portions_of(number_of, total, bound, slope, full):
    weights = [(1 << 20) // math.isqrt(grade ** slope) + 1 for grade in range(1, number_of + 1)]
    largest = bound if full else min(bound, max(-(-total // number_of), total * weights[0] // sum(weights)))
    least = 1 if total - largest >= number_of - 1 else 0
    given, surplus = [largest] + [least] * (number_of - 1), total - largest - least * (number_of - 1)
    while surplus > 0:
        free = [i for i in range(1, number_of) if given[i] < largest] or [i for i in range(1, number_of) if given[i] < bound]
        mass, budget = sum([weights[i] for i in free]), surplus
        for i in free:
            more = min(bound - given[i], max(1, budget * weights[i] // mass), surplus)
            given[i] = given[i] + more
            surplus = surplus - more
    return np.array(given)


def noise(key, shape, deviation, bound, cuts=(), kind=jnp.bfloat16):
    factor_of = steps_of(key, shape, cuts, -0.22, 0.18) if cuts else 1.0
    result = jax.random.normal(key, shape, jnp.float32) * deviation * factor_of
    return jnp.minimum(jnp.maximum(result, -bound), bound).astype(kind)


def setup_inputs(seed: int = 0) -> dict:
    arg_keys = jax.random.split(jax.random.key(seed), 6)
    out_grads = noise(arg_keys[0], (N_DP, TOK_EXP, D), 1.0, 6.0, ((0, 4), (1, 8)))
    expert_ids_keys = jax.random.split(jax.random.fold_in(arg_keys[1], 1), N_DP * TOK_EXP // TOK_DEV)
    expert_ids_turns = jax.random.permutation(jax.random.fold_in(arg_keys[1], 3), N_DP * TOK_EXP // TOK_DEV)
    expert_ids = jax.vmap(lambda own, number: routed_block(jax.random.fold_in(arg_keys[1], 2), own, number, TOK_DEV, EXPERTS, TOP, CAP, 1))(expert_ids_keys, expert_ids_turns).reshape((N_DP, TOK_EXP, TOP))
    gate_probs = jnp.clip(0.05 + 0.45 * jax.random.uniform(arg_keys[2], (N_DP, TOK_EXP, TOP), jnp.float32) ** steps_of(arg_keys[2], (N_DP, TOK_EXP, TOP), ((0, 4), (1, 8)), -0.2, 0.2), 0.05, 0.5)
    hidden_acts = noise(arg_keys[3], (N_DP, EXPERTS, SLOTS, FF), 1.0, 6.0, ((0, 4), (1, 8)))
    q_previous = noise(arg_keys[4], (EXPERTS, RANK, D), D ** -0.5, 0.0625, ((0, 8),))
    return {"out_grads": out_grads, "expert_ids": expert_ids, "gate_probs": gate_probs, "hidden_acts": hidden_acts, "q_previous": q_previous}


def to_half(values):
    return lax.optimization_barrier(values.astype(jnp.bfloat16))

def slot_tables(route_ids, gate_values, num_experts, capacity):
    flat_ids = route_ids.reshape(-1)
    row_count = flat_ids.shape[0]
    top_k = route_ids.shape[-1]
    one_hot = (flat_ids[:, None] == jnp.arange(num_experts, dtype=jnp.int32)[None, :]).astype(jnp.int32)
    earlier = jnp.cumsum(one_hot, axis=0) - one_hot
    position = lax.optimization_barrier(jnp.sum(earlier * one_hot, axis=1)).astype(jnp.int32)
    slot_index = (flat_ids * capacity + position).astype(jnp.int32)
    token_of = jnp.zeros((num_experts * capacity,), jnp.int32).at[slot_index].set((jnp.arange(row_count, dtype=jnp.int32) // top_k).astype(jnp.int32))
    gate_of = jnp.zeros((num_experts * capacity,), jnp.float32).at[slot_index].set(gate_values.reshape(-1).astype(jnp.float32))
    return (token_of, gate_of)

def reference(out_grads, expert_ids, gate_probs, hidden_acts, q_previous):
    grads_blocks = out_grads.reshape(N_DP, N_EXPERT, TOK_DEV, D)
    id_blocks = expert_ids.reshape(N_DP, N_EXPERT, TOK_DEV, TOP)
    gate_blocks = gate_probs.reshape(N_DP, N_EXPERT, TOK_DEV, TOP)
    tables = jax.vmap(jax.vmap(lambda ids, gts: slot_tables(ids, gts, EXPERTS, CAP)))
    token_of, gate_of = tables(id_blocks, gate_blocks)

    def pick_rows(grads_one, tokens_one):
        return jnp.take(grads_one, tokens_one, axis=0)

    def one_expert(expert_num):
        start = (expert_num * CAP).astype(jnp.int32)
        tokens_here = lax.dynamic_slice_in_dim(token_of, start, CAP, 2)
        gates_here = lax.dynamic_slice_in_dim(gate_of, start, CAP, 2)
        picked = jax.vmap(jax.vmap(pick_rows))(grads_blocks, tokens_here)
        routed = to_half(picked.astype(jnp.float32) * gates_here[..., None]).reshape(N_DP, SLOTS, D)
        hidden_here = lax.dynamic_index_in_dim(hidden_acts, expert_num, 1, keepdims=False)
        q_here = lax.dynamic_index_in_dim(q_previous, expert_num, 0, keepdims=False)
        mixed = to_half(jnp.einsum('psd,rd->psr', routed.astype(jnp.float32), q_here.astype(jnp.float32)))
        factor = jnp.einsum('psr,psf->rf', mixed.astype(jnp.float32), hidden_here.astype(jnp.float32))
        gram = jnp.dot(factor, factor.T, precision=lax.Precision.HIGHEST)
        lower = jnp.linalg.cholesky(gram)
        inverse = jax.scipy.linalg.solve_triangular(lower, jnp.eye(RANK, dtype=jnp.float32), lower=True)
        ortho = jnp.dot(inverse, factor, precision=lax.Precision.HIGHEST)
        ortho_half = to_half(ortho)
        projected = to_half(jnp.einsum('psf,rf->psr', hidden_here.astype(jnp.float32), ortho_half.astype(jnp.float32)))
        q_new = jnp.einsum('psr,psd->rd', projected.astype(jnp.float32), routed.astype(jnp.float32))
        return (ortho * math.sqrt(FF), q_new)
    new_basis, q_update = lax.map(one_expert, jnp.arange(EXPERTS, dtype=jnp.int32))
    return (new_basis, q_update)
```

```python
import functools
import math

import jax
import jax.numpy as jnp
from jax import lax
from jax.experimental import pallas as pl
from jax.experimental.pallas import tpu as pltpu
from jax.sharding import PartitionSpec as P

F32, BF16 = jnp.float32, jnp.bfloat16


def inverse_kernel(factor_ref, ortho_ref):
    count, rank, _ = factor_ref.shape
    rows = lax.broadcasted_iota(jnp.int32, (rank, 2 * rank), 0)
    cols = lax.broadcasted_iota(jnp.int32, (rank, 2 * rank), 1)
    eye = (cols == rows + rank).astype(F32)
    tables = []
    for j in range(count):
        value = factor_ref[j]
        doubled = jnp.concatenate([value, jnp.zeros_like(value)], axis=0)
        gram = lax.dot_general(
            value, doubled, (((1,), (1,)), ((), ())),
            precision=lax.Precision.HIGHEST, preferred_element_type=F32,
        )
        tables.append(gram + eye)
    for k in range(rank):
        for j in range(count):
            table = tables[j]
            row = table[k : k + 1, :]
            pivot = lax.rsqrt(row[:, k : k + 1])
            scaled = row * pivot
            column = table[:, k : k + 1] * pivot
            table = jnp.where(rows > k, table - column * scaled, table)
            tables[j] = jnp.where(rows == k, scaled, table)
    for j in range(count):
        ortho_ref[j] = jnp.dot(
            tables[j][:, rank:], factor_ref[j],
            precision=lax.Precision.HIGHEST, preferred_element_type=F32,
        ).astype(ortho_ref.dtype)


def orthonormal(factor):
    return pl.pallas_call(
        inverse_kernel,
        out_shape=jax.ShapeDtypeStruct(factor.shape, BF16),
        name="orthonormal",
    )(factor)


def local(out_grads, expert_ids, gate_probs, hidden_acts, q_previous):
    n_expert = lax.axis_size("expert")
    experts, slots, units = hidden_acts.shape[1:]
    capacity = slots // n_expert
    tokens, width = out_grads.shape[1:]
    rank = q_previous.shape[1]
    first = lax.axis_index("expert") * experts

    route = jnp.concatenate([expert_ids[0].astype(F32), gate_probs[0]], axis=1)
    route = lax.all_gather(route, "expert", axis=0)
    grads = lax.all_gather(out_grads[0], "expert", axis=0)
    top = expert_ids.shape[2]
    mine = (first + jnp.arange(experts)).astype(F32)
    hit = route[:, :, :top, None] == mine
    gate = jnp.sum(jnp.where(hit, route[:, :, top:, None], 0.0), axis=2)
    chosen = jnp.any(hit, axis=2)
    earlier = (jnp.arange(tokens)[:, None] > jnp.arange(tokens)[None, :]).astype(BF16)
    place = jnp.einsum("ut,btj->buj", earlier, chosen.astype(BF16), preferred_element_type=F32)
    place = jnp.where(chosen, place, -1.0).transpose(2, 0, 1)
    pick = (place[:, :, None, :] == jnp.arange(capacity, dtype=F32)[:, None]).astype(BF16)

    mixed = jnp.einsum("btd,jrd->btjr", grads, q_previous, preferred_element_type=F32)
    mixed = (mixed * gate[..., None]).astype(BF16)
    mixed = jnp.einsum("jbct,btjr->jbcr", pick, mixed, preferred_element_type=F32).astype(BF16)
    hidden = hidden_acts[0]
    factor = jnp.einsum(
        "jsr,jsf->jrf", mixed.reshape(experts, slots, rank), hidden, preferred_element_type=F32
    )
    share = lax.psum_scatter(factor, "dp", scatter_dimension=0, tiled=True)
    ortho = lax.all_gather(orthonormal(share), "dp", axis=0, tiled=True)
    projected = jnp.einsum("jsf,jrf->jsr", hidden, ortho, preferred_element_type=F32).astype(BF16)
    spread = jnp.einsum(
        "jbct,jbcr->btjr",
        pick,
        projected.reshape(experts, n_expert, capacity, rank),
        preferred_element_type=F32,
    )
    spread = (spread * gate[..., None]).astype(BF16)
    terms = jnp.einsum("btjr,btd->jrd", spread, grads, preferred_element_type=F32)
    q_update = lax.psum_scatter(
        terms.astype(BF16), "dp", scatter_dimension=2, tiled=True
    ).astype(F32)
    new_basis = ortho.astype(F32) * math.sqrt(units)
    return (new_basis, q_update)


def solution(mesh):
    return jax.shard_map(
        local,
        mesh=mesh,
        in_specs=(
            P("dp", "expert", None),
            P("dp", "expert", None),
            P("dp", "expert", None),
            P("dp", "expert", None, None),
            P("expert", None, None),
        ),
        out_specs=(P("expert", None, None), P("expert", None, "dp")),
        check_vma=False,
    )
```

```python
import functools
import math

import jax
import jax.numpy as jnp
from jax import lax
from jax.experimental import pallas as pl
from jax.experimental.pallas import tpu as pltpu
from jax.sharding import PartitionSpec as P

F32, BF16 = jnp.float32, jnp.bfloat16


MESH = pl.DeviceIdType.MESH


def orthonormal(value):
    rank = value[0].shape[0]
    rows = lax.broadcasted_iota(jnp.int32, (rank, 2 * rank), 0)
    cols = lax.broadcasted_iota(jnp.int32, (rank, 2 * rank), 1)
    eye = (cols == rows + rank).astype(F32)
    tables = []
    for one in value:
        doubled = jnp.concatenate([one, jnp.zeros_like(one)], axis=0)
        gram = lax.dot_general(
            one, doubled, (((1,), (1,)), ((), ())),
            precision=lax.Precision.HIGHEST, preferred_element_type=F32,
        )
        tables.append(gram + eye)
    for k in range(rank):
        for j, table in enumerate(tables):
            row = table[k : k + 1, :]
            pivot = lax.rsqrt(row[:, k : k + 1])
            scaled = row * pivot
            column = table[:, k : k + 1] * pivot
            table = jnp.where(rows > k, table - column * scaled, table)
            tables[j] = jnp.where(rows == k, scaled, table)
    return [
        jnp.dot(
            table[:, rank:], one, precision=lax.Precision.HIGHEST, preferred_element_type=F32
        )
        for table, one in zip(tables, value)
    ]


def factor_kernel(
    n, part_ref, hidden_ref, ortho_ref, proj_ref,
    hidden, got_part, fact, got_fact, load_sem, send_sem, recv_sem,
):
    me = lax.axis_index("dp")
    experts = hidden.shape[0]
    per = experts // n
    peers = [lax.rem(me + offset, n) for offset in range(1, n)]
    loads = []
    for j in range(experts):
        load = pltpu.make_async_copy(hidden_ref.at[j], hidden.at[j], load_sem.at[j])
        load.start()
        loads.append(load)
    barrier = pltpu.get_barrier_semaphore()
    for peer in peers:
        pl.semaphore_signal(barrier, inc=1, device_id={"dp": peer}, device_id_type=MESH)
    pl.semaphore_wait(barrier, n - 1)

    def push(phase, offset, source, target):
        copy = pltpu.make_async_remote_copy(
            src_ref=source,
            dst_ref=target,
            send_sem=send_sem.at[phase, offset],
            recv_sem=recv_sem.at[phase, offset],
            device_id={"dp": peers[offset]},
            device_id_type=MESH,
        )
        copy.start()
        return copy

    sent = [push(0, o, part_ref.at[peers[o]], got_part.at[o]) for o in range(n - 1)]
    for copy in sent:
        copy.wait()
    mixed = part_ref[me].astype(F32)
    for o in range(n - 1):
        mixed = mixed + got_part[o].astype(F32)
    mixed = mixed.astype(BF16)
    for load in loads:
        load.wait()
    rank = mixed.shape[1]
    for j in range(experts):
        fact[j] = jnp.dot(mixed[j], hidden[j], preferred_element_type=F32).astype(BF16)
    sent = [
        push(1, o, fact.at[pl.ds(peers[o] * per, per)], got_fact.at[o]) for o in range(n - 1)
    ]
    for copy in sent:
        copy.wait()
    share = []
    for i in range(per):
        total = fact[me * per + i].astype(F32)
        for o in range(n - 1):
            total = total + got_fact[o, i].astype(F32)
        share.append(total)
    for i, value in enumerate(orthonormal(share)):
        ortho_ref[me * per + i] = value.astype(BF16)
    mine = ortho_ref.at[pl.ds(me * per, per)]
    sent = [push(2, o, mine, mine) for o in range(n - 1)]

    def project(group):
        for i in range(per):
            j = group * per + i
            proj_ref[me, j] = lax.dot_general(
                ortho_ref[j], hidden[j], (((1,), (1,)), ((), ())), preferred_element_type=F32
            ).astype(BF16)

    project(me)
    for o in range(n - 1):
        sent[o].wait()
        project(lax.rem(me + n - 1 - o, n))
    sent = [push(3, o, proj_ref.at[me], proj_ref.at[me]) for o in range(n - 1)]
    for copy in sent:
        copy.wait()


def factors(part, hidden, n):
    experts, slots, units = hidden.shape
    rank = part.shape[2]
    per = experts // n
    vmem = pl.BlockSpec(memory_space=pltpu.VMEM)
    return pl.pallas_call(
        functools.partial(factor_kernel, n),
        out_shape=(
            jax.ShapeDtypeStruct((experts, rank, units), BF16),
            jax.ShapeDtypeStruct((n, experts, rank, slots), BF16),
        ),
        in_specs=[vmem, pl.BlockSpec(memory_space=pl.ANY)],
        out_specs=(vmem, vmem),
        scratch_shapes=[
            pltpu.VMEM((experts, slots, units), BF16),
            pltpu.VMEM((n - 1, experts, rank, slots), BF16),
            pltpu.VMEM((experts, rank, units), BF16),
            pltpu.VMEM((n - 1, per, rank, units), BF16),
            pltpu.SemaphoreType.DMA((experts,)),
            pltpu.SemaphoreType.DMA((4, n - 1)),
            pltpu.SemaphoreType.DMA((4, n - 1)),
        ],
        compiler_params=pltpu.CompilerParams(
            collective_id=0, has_side_effects=True, vmem_limit_bytes=40 * 2**20
        ),
        name="factors",
    )(part, hidden)


def gathered(grads):
    n_dp = lax.axis_size("dp")
    tokens, width = grads.shape
    split = grads.reshape(tokens, n_dp, width // n_dp).transpose(1, 0, 2)
    split = lax.all_to_all(split, "dp", split_axis=0, concat_axis=0, tiled=True)
    return lax.all_gather(split, "expert", axis=0)


def local(out_grads, expert_ids, gate_probs, hidden_acts, q_previous):
    n_expert = lax.axis_size("expert")
    n_dp = lax.axis_size("dp")
    experts, slots, units = hidden_acts.shape[1:]
    capacity = slots // n_expert
    tokens, width = out_grads.shape[1:]
    top = expert_ids.shape[2]
    rank = q_previous.shape[1]
    cols = width // n_dp
    first = lax.axis_index("expert") * experts

    route = jnp.concatenate([expert_ids[0].astype(F32), gate_probs[0]], axis=1)
    route = lax.all_gather(route, ("dp", "expert"), axis=0)
    route = route.reshape(n_dp, n_expert, tokens, 2 * top)
    grads = gathered(out_grads[0])
    mine = (first + jnp.arange(experts)).astype(F32)[:, None]
    ids = route[..., :top].transpose(3, 0, 1, 2)[:, :, :, None, :]
    weight = route[..., top:].transpose(3, 0, 1, 2)[:, :, :, None, :]
    hit = ids == mine
    gate = jnp.sum(jnp.where(hit, weight, 0.0), axis=0)
    chosen = jnp.any(hit, axis=0)
    earlier = (jnp.arange(tokens)[:, None] < jnp.arange(tokens)[None, :]).astype(BF16)
    place = jnp.einsum("pbjt,tu->pbju", chosen.astype(BF16), earlier, preferred_element_type=F32)
    place = jnp.where(chosen, place, -1.0)
    pick = (place[:, :, :, None, :] == jnp.arange(capacity, dtype=F32)[:, None]).astype(BF16)

    q_part = lax.dynamic_slice_in_dim(q_previous, lax.axis_index("dp") * cols, cols, 2)
    mixed = jnp.einsum("jrd,bptd->jrbpt", q_part, grads, preferred_element_type=F32)
    scale = gate.transpose(2, 1, 0, 3)
    mixed = (mixed * scale[:, None]).astype(BF16)
    part = jnp.einsum("jrbpt,pbjct->pjrbc", mixed, pick, preferred_element_type=F32).astype(BF16)
    part = part.reshape(n_dp, experts, rank, slots)
    ortho, proj = factors(part, hidden_acts[0], n_dp)
    proj = proj.reshape(n_dp, experts, rank, n_expert, capacity)
    spread = jnp.einsum("pjrbc,pbjct->jrbpt", proj, pick, preferred_element_type=F32)
    spread = (spread * scale[:, None]).astype(BF16)
    q_update = jnp.einsum("jrbpt,bptd->jrd", spread, grads, preferred_element_type=F32)
    new_basis = ortho.astype(F32) * math.sqrt(units)
    return (new_basis, q_update)


def solution(mesh):
    return jax.shard_map(
        local,
        mesh=mesh,
        in_specs=(
            P("dp", "expert", None),
            P("dp", "expert", None),
            P("dp", "expert", None),
            P("dp", "expert", None, None),
            P("expert", None, None),
        ),
        out_specs=(P("expert", None, None), P("expert", None, "dp")),
        check_vma=False,
    )
```

```python
import functools
import math

import jax
import jax.numpy as jnp
from jax import lax
from jax.experimental import pallas as pl
from jax.experimental.pallas import tpu as pltpu
from jax.sharding import PartitionSpec as P

F32, BF16 = jnp.float32, jnp.bfloat16


MESH = pl.DeviceIdType.MESH


def orthonormal(value):
    rank = value[0].shape[0]
    rows = lax.broadcasted_iota(jnp.int32, (rank, 2 * rank), 0)
    cols = lax.broadcasted_iota(jnp.int32, (rank, 2 * rank), 1)
    eye = (cols == rows + rank).astype(F32)
    tables = []
    for one in value:
        doubled = jnp.concatenate([one, jnp.zeros_like(one)], axis=0)
        gram = lax.dot_general(
            one, doubled, (((1,), (1,)), ((), ())),
            precision=lax.Precision.HIGHEST, preferred_element_type=F32,
        )
        tables.append(gram + eye)
    for k in range(rank):
        for j, table in enumerate(tables):
            row = table[k : k + 1, :]
            pivot = lax.rsqrt(row[:, k : k + 1])
            scaled = row * pivot
            column = table[:, k : k + 1] * pivot
            table = jnp.where(rows > k, table - column * scaled, table)
            tables[j] = jnp.where(rows == k, scaled, table)
    return [
        jnp.dot(
            table[:, rank:], one, precision=lax.Precision.HIGHEST, preferred_element_type=F32
        )
        for table, one in zip(tables, value)
    ]


def factor_kernel(
    n, part_ref, hidden_ref, ortho_ref, proj_ref,
    hidden, got_part, fact, got_fact, load_sem, send_sem, recv_sem,
):
    me = lax.axis_index("dp")
    experts = hidden.shape[0]
    per = experts // n
    peers = [lax.rem(me + offset, n) for offset in range(1, n)]
    loads = []
    for j in range(experts):
        load = pltpu.make_async_copy(hidden_ref.at[j], hidden.at[j], load_sem.at[j])
        load.start()
        loads.append(load)
    barrier = pltpu.get_barrier_semaphore()
    for peer in peers:
        pl.semaphore_signal(barrier, inc=1, device_id={"dp": peer}, device_id_type=MESH)
    pl.semaphore_wait(barrier, n - 1)

    def push(phase, offset, source, target):
        copy = pltpu.make_async_remote_copy(
            src_ref=source,
            dst_ref=target,
            send_sem=send_sem.at[phase, offset],
            recv_sem=recv_sem.at[phase, offset],
            device_id={"dp": peers[offset]},
            device_id_type=MESH,
        )
        copy.start()
        return copy

    sent = [push(0, o, part_ref.at[peers[o]], got_part.at[o]) for o in range(n - 1)]
    for copy in sent:
        copy.wait()
    mixed = part_ref[me].astype(F32)
    for o in range(n - 1):
        mixed = mixed + got_part[o].astype(F32)
    mixed = mixed.astype(BF16)
    for load in loads:
        load.wait()
    rank = mixed.shape[1]
    for j in range(experts):
        fact[j] = jnp.dot(mixed[j], hidden[j], preferred_element_type=F32).astype(BF16)
    sent = [
        push(1, o, fact.at[pl.ds(peers[o] * per, per)], got_fact.at[o]) for o in range(n - 1)
    ]
    for copy in sent:
        copy.wait()
    share = []
    for i in range(per):
        total = fact[me * per + i].astype(F32)
        for o in range(n - 1):
            total = total + got_fact[o, i].astype(F32)
        share.append(total)
    for i, value in enumerate(orthonormal(share)):
        ortho_ref[me * per + i] = value.astype(BF16)
    mine = ortho_ref.at[pl.ds(me * per, per)]
    sent = [push(2, o, mine, mine) for o in range(n - 1)]

    def project(group):
        for i in range(per):
            j = group * per + i
            proj_ref[me, j] = lax.dot_general(
                ortho_ref[j], hidden[j], (((1,), (1,)), ((), ())), preferred_element_type=F32
            ).astype(BF16)

    project(me)
    for o in range(n - 1):
        sent[o].wait()
        project(lax.rem(me + n - 1 - o, n))
    sent = [push(3, o, proj_ref.at[me], proj_ref.at[me]) for o in range(n - 1)]
    for copy in sent:
        copy.wait()


def factors(part, hidden, n):
    experts, slots, units = hidden.shape
    rank = part.shape[2]
    per = experts // n
    vmem = pl.BlockSpec(memory_space=pltpu.VMEM)
    return pl.pallas_call(
        functools.partial(factor_kernel, n),
        out_shape=(
            jax.ShapeDtypeStruct((experts, rank, units), BF16),
            jax.ShapeDtypeStruct((n, experts, rank, slots), BF16),
        ),
        in_specs=[vmem, pl.BlockSpec(memory_space=pl.ANY)],
        out_specs=(vmem, vmem),
        scratch_shapes=[
            pltpu.VMEM((experts, slots, units), BF16),
            pltpu.VMEM((n - 1, experts, rank, slots), BF16),
            pltpu.VMEM((experts, rank, units), BF16),
            pltpu.VMEM((n - 1, per, rank, units), BF16),
            pltpu.SemaphoreType.DMA((experts,)),
            pltpu.SemaphoreType.DMA((4, n - 1)),
            pltpu.SemaphoreType.DMA((4, n - 1)),
        ],
        compiler_params=pltpu.CompilerParams(
            collective_id=0, has_side_effects=True, vmem_limit_bytes=40 * 2**20
        ),
        name="factors",
    )(part, hidden)


def gather_kernel(
    n_expert, n_dp, x_ref, all_ref,
    own_sem, z_send, z_recv, one_send, one_recv, two_send, two_recv, core_send, core_recv,
):
    me, z = lax.axis_index("expert"), lax.axis_index("dp")
    chips = n_expert // 2
    wide = math.isqrt(chips)
    sides = (wide, chips // wide)
    core, chip = lax.rem(me, 2), me // 2
    spot = (lax.rem(chip, wide), chip // wide)
    half, cols = x_ref.shape[0] // 2, all_ref.shape[3]

    def shifted(dim, by):
        return lax.rem(spot[dim] + by + sides[dim], sides[dim])

    def block(x, y, c):
        return (y * wide + x) * 2 + c

    def neighbour(dim, by):
        moved = shifted(dim, by)
        return block(moved, spot[1], core) if dim == 0 else block(spot[0], moved, core)

    def source(dim, first, second, c):
        x, y = (first, second) if dim == 0 else (second, first)
        return block(shifted(0, -x), shifted(1, -y), c)

    barrier = pltpu.get_barrier_semaphore()
    greeted = [{"dp": lax.rem(z + k, n_dp)} for k in range(1, n_dp)]
    greeted += [{"expert": neighbour(d, by)} for d in range(2) for by in range(1, sides[d])]
    greeted += [{"expert": block(spot[0], spot[1], 1 - core)}]
    for peer in greeted:
        pl.semaphore_signal(barrier, inc=1, device_id=peer, device_id_type=MESH)
    pl.semaphore_wait(barrier, len(greeted))

    sent = []

    def push(src, dst, send_sem, recv_sem, device):
        copy = pltpu.make_async_remote_copy(
            src_ref=src, dst_ref=dst, send_sem=send_sem, recv_sem=recv_sem,
            device_id=device, device_id_type=MESH,
        )
        copy.start()
        sent.append(copy)
        return copy

    def columns(r):
        return x_ref.at[:, pl.ds(pl.multiple_of(r * cols, 128), cols)]

    own = pltpu.make_async_copy(columns(z), all_ref.at[me, z], own_sem)
    own.start()
    arrive_z, arrive_one, arrive_two, arrive_core = {}, {}, {}, []
    for k in range(1, n_dp):
        to = lax.rem(z + k, n_dp)
        arrive_z[k] = push(
            columns(to), all_ref.at[me, z], z_send.at[k - 1], z_recv.at[k - 1], {"dp": to}
        )

    def rows(b, k, h):
        return all_ref.at[b, lax.rem(z - k + n_dp, n_dp), pl.ds(h * half, half)]

    def swap(k, h, first, second):
        part = rows(source(h, first, second, core), k, h)
        at = (h, k, first, second)
        partner = {"expert": block(spot[0], spot[1], 1 - core)}
        arrive_core.append(push(part, part, core_send.at[at], core_recv.at[at], partner))

    def onward(k, h, first):
        part = rows(source(h, first, 0, core), k, h)
        for by in range(1, sides[1 - h]):
            at = (h, k, first, by - 1)
            arrive_two[at] = push(
                part, part, two_send.at[at], two_recv.at[at], {"expert": neighbour(1 - h, by)}
            )
        swap(k, h, first, 0)

    for k in range(n_dp + 2):
        if k < n_dp:
            if k:
                arrive_z[k].wait_recv()
            else:
                own.wait()
            for h in range(2):
                part = rows(me, k, h)
                for by in range(1, sides[h]):
                    at = (h, k, by - 1)
                    arrive_one[at] = push(
                        part, part, one_send.at[at], one_recv.at[at], {"expert": neighbour(h, by)}
                    )
            for h in range(2):
                onward(k, h, 0)
        if 0 <= k - 1 < n_dp:
            for h in range(2):
                for by in range(1, sides[h]):
                    arrive_one[(h, k - 1, by - 1)].wait_recv()
                    onward(k - 1, h, by)
        if 0 <= k - 2 < n_dp:
            for h in range(2):
                for first in range(sides[h]):
                    for by in range(1, sides[1 - h]):
                        arrive_two[(h, k - 2, first, by - 1)].wait_recv()
                        swap(k - 2, h, first, by)
    for copy in arrive_core:
        copy.wait_recv()
    for copy in sent:
        copy.wait_send()


def gathered(grads):
    n_expert, n_dp = lax.axis_size("expert"), lax.axis_size("dp")
    tokens, width = grads.shape
    long = max(math.isqrt(n_expert // 2), n_expert // 2 // math.isqrt(n_expert // 2))
    dma = pltpu.SemaphoreType.DMA
    return pl.pallas_call(
        functools.partial(gather_kernel, n_expert, n_dp),
        out_shape=jax.ShapeDtypeStruct((n_expert, n_dp, tokens, width // n_dp), grads.dtype),
        in_specs=[pl.BlockSpec(memory_space=pltpu.VMEM)],
        out_specs=pl.BlockSpec(memory_space=pl.ANY),
        scratch_shapes=[
            dma(()), dma((n_dp - 1,)), dma((n_dp - 1,)),
            dma((2, n_dp, long)), dma((2, n_dp, long)),
            dma((2, n_dp, long, long)), dma((2, n_dp, long, long)),
            dma((2, n_dp, long, long)), dma((2, n_dp, long, long)),
        ],
        compiler_params=pltpu.CompilerParams(
            collective_id=1, has_side_effects=True, vmem_limit_bytes=56 * 2**20
        ),
        name="gather_rows",
    )(grads)


def local(out_grads, expert_ids, gate_probs, hidden_acts, q_previous):
    n_expert = lax.axis_size("expert")
    n_dp = lax.axis_size("dp")
    experts, slots, units = hidden_acts.shape[1:]
    capacity = slots // n_expert
    tokens, width = out_grads.shape[1:]
    top = expert_ids.shape[2]
    rank = q_previous.shape[1]
    cols = width // n_dp
    first = lax.axis_index("expert") * experts

    route = jnp.concatenate([expert_ids[0].astype(F32), gate_probs[0]], axis=1)
    route = lax.all_gather(route, ("dp", "expert"), axis=0)
    route = route.reshape(n_dp, n_expert, tokens, 2 * top)
    grads = gathered(out_grads[0])
    mine = (first + jnp.arange(experts)).astype(F32)[:, None]
    ids = route[..., :top].transpose(3, 0, 1, 2)[:, :, :, None, :]
    weight = route[..., top:].transpose(3, 0, 1, 2)[:, :, :, None, :]
    hit = ids == mine
    gate = jnp.sum(jnp.where(hit, weight, 0.0), axis=0)
    chosen = jnp.any(hit, axis=0)
    earlier = (jnp.arange(tokens)[:, None] < jnp.arange(tokens)[None, :]).astype(BF16)
    place = jnp.einsum("pbjt,tu->pbju", chosen.astype(BF16), earlier, preferred_element_type=F32)
    place = jnp.where(chosen, place, -1.0)
    pick = (place[:, :, :, None, :] == jnp.arange(capacity, dtype=F32)[:, None]).astype(BF16)

    q_part = lax.dynamic_slice_in_dim(q_previous, lax.axis_index("dp") * cols, cols, 2)
    mixed = jnp.einsum("jrd,bptd->jrbpt", q_part, grads, preferred_element_type=F32)
    scale = gate.transpose(2, 1, 0, 3)
    mixed = (mixed * scale[:, None]).astype(BF16)
    part = jnp.einsum("jrbpt,pbjct->pjrbc", mixed, pick, preferred_element_type=F32).astype(BF16)
    part = part.reshape(n_dp, experts, rank, slots)
    ortho, proj = factors(part, hidden_acts[0], n_dp)
    proj = proj.reshape(n_dp, experts, rank, n_expert, capacity)
    spread = jnp.einsum("pjrbc,pbjct->jrbpt", proj, pick, preferred_element_type=F32)
    spread = (spread * scale[:, None]).astype(BF16)
    q_update = jnp.einsum("jrbpt,bptd->jrd", spread, grads, preferred_element_type=F32)
    new_basis = ortho.astype(F32) * math.sqrt(units)
    return (new_basis, q_update)


def solution(mesh):
    return jax.shard_map(
        local,
        mesh=mesh,
        in_specs=(
            P("dp", "expert", None),
            P("dp", "expert", None),
            P("dp", "expert", None),
            P("dp", "expert", None, None),
            P("expert", None, None),
        ),
        out_specs=(P("expert", None, None), P("expert", None, "dp")),
        check_vma=False,
    )
```
